32 devices in a mesh: expert: 8 (over y, x, core), hidden: 4 (over z).
Axes of the slice: x: 2, y: 2, z: 4, core: 2. Of those that a mesh axis runs over, the one named last changes fastest.
Arguments:
- tokens: bfloat16 [1024, 4096], P('expert', 'hidden'), may hold values from -6 to 6
- w_down: bfloat16 [4096, 1024], P('hidden', 'expert'), may hold values from -0.09375 to 0.09375
- w1_values: bfloat16 [32, 1024, 2688], P('expert', None, 'hidden'), may hold values from -0.1875 to 0.1875
- w1_scales: float32 [32, 8, 2688], P('expert', None, 'hidden'), may hold values from 0.5 to 2
- w2_values: bfloat16 [32, 2688, 1024], P('expert', 'hidden'), may hold values from -0.125 to 0.125
- w2_scales: float32 [32, 2688, 8], P('expert', 'hidden'), may hold values from 0.5 to 2
- w_up: bfloat16 [1024, 4096], P('expert', 'hidden'), may hold values from -0.1875 to 0.1875
- expert_ids: int32 [1024, 6], P('expert'), may hold values from 0 to 31, all different within a row; in each aligned block of 128 rows (0 to 127, 128 to 255, ...) at most 32 rows name the same one
- weight_codes: int32 [1024, 6], P('expert'), may hold values from 1 to 255
Outputs:
- mixed: bfloat16 [1024, 4096], P('expert', 'hidden')
The draws below stay inside these ranges and needn't reach their ends.
Inputs may be any that keep to these rules, and one draw needn't show every extreme that they name: `expert_ids`: each row names 6 different experts. Within each aligned block of 128 rows (the rows of one index of expert) no expert is named more than 32 times.
All inputs are finite; a program needn't handle non-finite values.
Results may differ from the reference program's by a relative error of at most 0.03.
Values may be sent and summed in bfloat16 or wider, within the bound.
No kernel may reach another device: no remote copies, remote signals or barrier semaphores. Data moves between devices by JAX's collectives and lax.ppermute only.
A program may use at most 128 MiB of HBM per device.

```python
import math
import jax
import jax.numpy as jnp
import numpy as np
from jax import lax

D = 4096
LATENT = 1024
FF = 2688
BLK = 128
TOP = 6
TOK_DEV = 128
EXPERTS = 32
TOKENS = 1024
CAP = 32
SLOTS = 256
N_EXPERT = 8
N_HIDDEN = 4


def plant(drawn, rng, least, high):
    dims = drawn.shape
    index_at = [jax.random.randint(jax.random.fold_in(rng, axis), (), 0, dims[axis]) for axis in range(len(dims))]
    drawn = drawn.at[tuple(index_at)].set(least)
    longest = dims.index(max(dims))
    index_at[longest] = (index_at[longest] + 1) % dims[longest]
    return drawn.at[tuple(index_at)].set(high)


def block_scale(own_key, extent, pieces, smallest, top_value):
    def one(axis_at, parts):
        heights = jax.random.uniform(jax.random.fold_in(jax.random.fold_in(own_key, 6), axis_at), (parts,), jnp.float32, smallest / len(pieces), top_value / len(pieces))
        return jnp.repeat(jnp.exp(heights), extent[axis_at] // parts).reshape((-1,) + (1,) * (len(extent) - axis_at - 1))

    factor_of = one(*pieces[0])
    for cut in pieces[1:]:
        factor_of = factor_of * one(*cut)
    return factor_of


def shared_out(own_key, own, number, rows, number_of, top, limit, skew):
    ranking = jax.random.permutation(own_key, number_of)
    heavy_load, ordinary = shares(number_of, rows * top, limit, skew, True), shares(number_of, rows * top, limit, skew, False)
    places = jnp.arange(number_of)

    def named(sizes, turn):
        used = int((sizes > 0).sum())
        fixed = max(1, used // 4)
        passed = fixed + (places - fixed + turn * (used - fixed)) % max(1, number_of - fixed)
        return jnp.zeros((number_of,), jnp.int32).at[ranking[jnp.where(places < fixed, places, passed)]].set(jnp.asarray(sizes, jnp.int32))

    sizes = jnp.where(number % 4 == 0, named(heavy_load, number // 4), named(ordinary, number - number // 4 - 1))
    mixed = jax.random.permutation(jax.random.fold_in(own, 3), number_of)
    source_of, receiver = mixed[0:number_of // 2 * 2:2], mixed[1:number_of // 2 * 2:2]
    margin = jnp.minimum(sizes[source_of] - 1, limit - sizes[receiver]) // 2
    margin = jnp.where((source_of == ranking[0]) | (receiver == ranking[0]) | (sizes[receiver] == 0), 0, jnp.maximum(margin, 0))
    passed = jax.random.randint(jax.random.fold_in(own, 4), (number_of // 2,), 0, 1 << 20) % (margin + 1)
    sizes = sizes.at[source_of].add(-passed).at[receiver].add(passed)
    labels = jnp.searchsorted(jnp.cumsum(sizes), jnp.arange(rows * top), side="right").astype(jnp.int32)
    listing = labels.reshape(top, rows).T
    listing = listing[jax.random.permutation(jax.random.fold_in(own, 1), rows)]
    turn = jax.random.randint(jax.random.fold_in(own, 2), (rows, 1), 0, top)
    return jnp.take_along_axis(listing, (jnp.arange(top)[None, :] + turn) % top, axis=1)


def shares(number_of, total, bound, skew, full):
    weights = [(1 << 20) // math.isqrt(rank ** skew) + 1 for rank in range(1, number_of + 1)]
    largest = bound if full else min(bound, max(-(-total // number_of), total * weights[0] // sum(weights)))
    least = 1 if total - largest >= number_of - 1 else 0
    given, surplus = [largest] + [least] * (number_of - 1), total - largest - least * (number_of - 1)
    while surplus > 0:
        free = [i for i in range(1, number_of) if given[i] < largest] or [i for i in range(1, number_of) if given[i] < bound]
        mass, budget = sum([weights[i] for i in free]), surplus
        for i in free:
            addition = min(bound - given[i], max(1, budget * weights[i] // mass), surplus)
            given[i] = given[i] + addition
            surplus = surplus - addition
    return np.array(given)


def gaussian(rng, dims, scale, limit, cuts=(), kind=jnp.bfloat16):
    drawn = scale * jax.random.normal(rng, dims, jnp.float32)
    if cuts:
        drawn = drawn * block_scale(rng, dims, cuts, -0.22, 0.18)
    return jnp.clip(drawn, -limit, limit).astype(kind)


def setup_inputs(seed: int = 0) -> dict:
    arg_keys = jax.random.split(jax.random.key(seed), 10)
    tokens = gaussian(arg_keys[0], (TOKENS, D), 1.0, 6.0, ((0, 8), (1, 4)))
    w_down = gaussian(arg_keys[1], (D, LATENT), D ** -0.5, 0.09375, ((0, 4), (1, 8)))
    w1_values = gaussian(arg_keys[2], (EXPERTS, LATENT, FF), LATENT ** -0.5, 0.1875, ((0, 8), (2, 4)))
    w1_scales = jnp.clip(jnp.exp(math.log(2.0) - 1.3862944 * jax.random.uniform(arg_keys[3], (EXPERTS, LATENT // BLK, FF), jnp.float32) ** block_scale(arg_keys[3], (EXPERTS, LATENT // BLK, FF), ((0, 8), (2, 4)), -0.2, 0.2)), 0.5, 2.0)
    w2_values = gaussian(arg_keys[4], (EXPERTS, FF, LATENT), FF ** -0.5, 0.125, ((0, 8), (1, 4)))
    w2_scales = jnp.clip(jnp.exp(math.log(2.0) - 1.3862944 * jax.random.uniform(arg_keys[5], (EXPERTS, FF, LATENT // BLK), jnp.float32) ** block_scale(arg_keys[5], (EXPERTS, FF, LATENT // BLK), ((0, 8), (1, 4)), -0.2, 0.2)), 0.5, 2.0)
    w_up = gaussian(arg_keys[6], (LATENT, D), LATENT ** -0.5, 0.1875, ((0, 8), (1, 4)))
    expert_ids_keys = jax.random.split(jax.random.fold_in(arg_keys[7], 1), TOKENS // TOK_DEV)
    expert_ids_turns = jax.random.permutation(jax.random.fold_in(arg_keys[7], 3), TOKENS // TOK_DEV)
    expert_ids = jax.vmap(lambda own, number: shared_out(jax.random.fold_in(arg_keys[7], 2), own, number, TOK_DEV, EXPERTS, TOP, CAP, 2))(expert_ids_keys, expert_ids_turns).reshape((TOKENS, TOP))
    weight_codes = plant(jax.random.randint(arg_keys[8], (TOKENS, TOP), 1, 256), jax.random.fold_in(arg_keys[8], 1), 1, 255).astype(jnp.int32)
    return {"tokens": tokens, "w_down": w_down, "w1_values": w1_values, "w1_scales": w1_scales, "w2_values": w2_values, "w2_scales": w2_scales, "w_up": w_up, "expert_ids": expert_ids, "weight_codes": weight_codes}


def block_positions(id_block):
    count = id_block.shape[0]
    order = jnp.arange(count, dtype=jnp.int32)
    matches = id_block[:, None] == id_block[None, :]
    before = order[:, None] > order[None, :]
    return jnp.sum((matches & before).astype(jnp.int32), axis=1).astype(jnp.int32)


def run_expert(operands):
    slot_rows, up_values, up_scales, down_values, down_scales = operands
    up_weight = (up_values.reshape(LATENT // BLK, BLK, FF).astype(jnp.float32) * up_scales[:, None, :]).reshape(LATENT, FF).astype(jnp.bfloat16)
    down_weight = (down_values.reshape(FF, LATENT // BLK, BLK).astype(jnp.float32) * down_scales[:, :, None]).reshape(FF, LATENT).astype(jnp.bfloat16)
    hidden_pre = jnp.dot(slot_rows.astype(jnp.float32), up_weight.astype(jnp.float32))
    activation = jnp.square(jnp.maximum(hidden_pre, 0.0)).astype(jnp.bfloat16)
    group_units = FF // N_HIDDEN
    grouped_act = activation.reshape(SLOTS, N_HIDDEN, group_units).astype(jnp.float32)
    grouped_down = down_weight.reshape(N_HIDDEN, group_units, LATENT).astype(jnp.float32)
    partial_value = jnp.einsum("shf,hfl->hsl", grouped_act, grouped_down).astype(jnp.bfloat16)
    return jnp.sum(partial_value.astype(jnp.float32), axis=0)


def reference(tokens, w_down, w1_values, w1_scales, w2_values, w2_scales, w_up, expert_ids, weight_codes):
    latent = jnp.dot(tokens, w_down, preferred_element_type=jnp.float32).astype(jnp.bfloat16)
    id_blocks = expert_ids.reshape(N_EXPERT, TOK_DEV * TOP)
    position = lax.map(block_positions, id_blocks).reshape(-1)
    flat_ids = expert_ids.reshape(-1).astype(jnp.int32)
    pair_index = jnp.arange(TOKENS * TOP, dtype=jnp.int32)
    token_index = (pair_index // TOP).astype(jnp.int32)
    source_index = (token_index // TOK_DEV).astype(jnp.int32)
    global_slot = (flat_ids * SLOTS + source_index * CAP + position).astype(jnp.int32)
    slot_table = jnp.full((EXPERTS * SLOTS,), TOKENS, dtype=jnp.int32).at[global_slot].set(token_index)
    padded = jnp.concatenate([latent, jnp.zeros((1, LATENT), dtype=jnp.bfloat16)], axis=0)
    rows = padded[slot_table].reshape(EXPERTS, SLOTS, LATENT)
    expert_out = lax.map(run_expert, (rows, w1_values, w1_scales, w2_values, w2_scales))
    picked = expert_out.reshape(EXPERTS * SLOTS, LATENT)[global_slot].reshape(TOKENS, TOP, LATENT).astype(jnp.float32)
    code_values = weight_codes.astype(jnp.float32)
    gate = code_values / jnp.sum(code_values, axis=1, keepdims=True)
    combined = jnp.sum(picked * gate[:, :, None], axis=1).astype(jnp.bfloat16)
    return jnp.dot(combined, w_up, preferred_element_type=jnp.float32).astype(jnp.bfloat16)
```

```python
import functools

import jax
import jax.numpy as jnp
from jax import lax
from jax.experimental import pallas as pl
from jax.experimental.pallas import tpu as pltpu
from jax.sharding import PartitionSpec as P


LANES = 128
MIB = 1 << 20
VMEM = pl.BlockSpec(memory_space=pltpu.VMEM)
SMEM = pl.BlockSpec(memory_space=pltpu.SMEM)
NT = (((1,), (1,)), ((), ()))


def params(mib, **more):
    return pltpu.CompilerParams(vmem_limit_bytes=mib * MIB, **more)


def at(block, width):
    return pl.ds(pl.multiple_of(block * width, width), width)


def scale_kernel(values_ref, scales_ref, out_ref):
    blocks = scales_ref.shape[2]
    width = values_ref.shape[2] // blocks
    for b in range(blocks):
        columns = slice(b * width, (b + 1) * width)
        scaled = values_ref[0, :, columns].astype(jnp.float32) * scales_ref[0, :, b : b + 1]
        out_ref[0, :, columns] = scaled.astype(out_ref.dtype)


def scale_weights(values, scales):
    count, units, latent = values.shape
    blocks = scales.shape[2]
    return pl.pallas_call(
        scale_kernel,
        grid=(count,),
        in_specs=[
            pl.BlockSpec((1, units, latent), lambda i: (i, 0, 0)),
            pl.BlockSpec((1, units, blocks), lambda i: (i, 0, 0)),
        ],
        out_specs=pl.BlockSpec((1, units, latent), lambda i: (i, 0, 0)),
        out_shape=jax.ShapeDtypeStruct(values.shape, values.dtype),
        compiler_params=params(24),
        cost_estimate=pl.CostEstimate(
            flops=8 * values.size, bytes_accessed=4 * values.size, transcendentals=0
        ),
        name="scale_weights",
    )(values, scales)


def latent_kernel(where_ref, *refs):
    planes = (len(refs) - 4) // 2
    del planes
    token_refs, weight_refs, out_refs = refs[:4], refs[4:-4], refs[-4:]
    plane, spot, line = where_ref[0], where_ref[1], where_ref[2]
    scratch = None
    del scratch
    for rel in range(4):
        goes = (spot ^ rel) ^ line
        for dy, weight_ref in enumerate(weight_refs):
            value = jnp.dot(
                token_refs[rel][...], weight_ref[...], preferred_element_type=jnp.float32
            ).astype(jnp.bfloat16)
            width = weight_ref.shape[1]
            for k in range(4):
                @pl.when(goes == k)
                def _():
                    out_refs[k][:, at(plane ^ dy, width)] = value


def latents(where, tokens, weights):
    rows, width = tokens[0].shape[0], weights[0].shape[1]
    shape = jax.ShapeDtypeStruct((rows, width * len(weights)), jnp.bfloat16)
    return pl.pallas_call(
        latent_kernel,
        in_specs=[SMEM] + [VMEM] * (4 + len(weights)),
        out_specs=[VMEM] * 4,
        out_shape=[shape] * 4,
        compiler_params=params(16),
        cost_estimate=pl.CostEstimate(flops=1 << 30, bytes_accessed=3 * MIB, transcendentals=0),
        name="latents",
    )(where, *tokens, *weights)


def routing_kernel(chosen, capacity, count, where_ref, *refs):
    meta_refs, select_ref, gates_ref = refs[:-2], refs[-2], refs[-1]
    owner, me = where_ref[3], where_ref[3]
    tokens = select_ref.shape[2]
    first = me * count
    row_of = lax.broadcasted_iota(jnp.int32, (tokens, tokens), 0)
    column_of = lax.broadcasted_iota(jnp.int32, (tokens, tokens), 1)
    earlier = (row_of < column_of).astype(jnp.bfloat16)
    place = lax.broadcasted_iota(jnp.int32, (capacity, tokens), 0).astype(jnp.float32)
    for rel, meta_ref in enumerate(meta_refs):
        rows = meta_ref.shape[0] - 16
        table = meta_ref[rows:, 0:tokens].astype(jnp.float32)
        ids, codes = table[0:chosen], table[chosen : 2 * chosen]
        gate = codes / jnp.sum(codes, axis=0, keepdims=True)
        picks, gate_of = [], []
        for j in range(count):
            hit = (ids == (first + j).astype(jnp.float32)).astype(jnp.float32)
            picks.append(jnp.sum(hit, axis=0, keepdims=True))
            gate_of.append(jnp.sum(hit * gate, axis=0, keepdims=True))
        picked = jnp.concatenate(picks, axis=0)
        position = jnp.dot(
            picked.astype(jnp.bfloat16), earlier, preferred_element_type=jnp.float32
        )
        select, gated = [], []
        for j in range(count):
            one = jnp.where(
                (place == position[j : j + 1]) & (picked[j : j + 1] > 0.5), 1.0, 0.0
            )
            select.append(one)
            gated.append(one * gate_of[j])
        source = owner ^ rel
        select_ref[source] = jnp.concatenate(select, axis=0).astype(jnp.bfloat16)
        gates_ref[source] = jnp.concatenate(gated, axis=0).T.astype(jnp.bfloat16)


def routing(where, metas, tokens, chosen, capacity, count):
    owners = len(metas)
    return pl.pallas_call(
        functools.partial(routing_kernel, chosen, capacity, count),
        in_specs=[SMEM] + [VMEM] * owners,
        out_specs=[VMEM] * 2,
        out_shape=[
            jax.ShapeDtypeStruct((owners, count * capacity, tokens), jnp.bfloat16),
            jax.ShapeDtypeStruct((owners, tokens, count * capacity), jnp.bfloat16),
        ],
        compiler_params=params(16),
        cost_estimate=pl.CostEstimate(flops=1 << 30, bytes_accessed=3 * MIB, transcendentals=0),
        name="routing",
    )(where, *metas)


def expert_kernel(sides, capacity, where_ref, *refs):
    pieces = refs[: 4 * sides]
    select_ref, gates_ref, up_ref, down_ref = refs[4 * sides : 4 * sides + 4]
    out_refs = refs[4 * sides + 4 : -2]
    rows_ref, terms_ref = refs[-2:]
    plane, spot, line = where_ref[0], where_ref[1], where_ref[2]
    planes = sides // 2
    count = rows_ref.shape[0]
    step = pl.program_id(0)
    width = pieces[0].shape[1] // planes

    @pl.when(step == 0)
    def _():
        for dy in range(planes):
            for k in range(4):
                source = (plane ^ dy) * 4 + (k ^ line)
                select = select_ref[source]
                for rel in range(4):
                    base = 2 * (dy * 4 + rel)
                    piece = pieces[base][...] if k == 0 else pieces[base + 1][k - 1]
                    got = jnp.dot(select, piece, preferred_element_type=jnp.float32)
                    got = got.astype(jnp.bfloat16)
                    for side in range(planes):
                        columns = at(side * 4 + (spot ^ rel), width)
                        for j in range(count):
                            rows_ref[
                                j, (dy * 4 + k) * capacity : (dy * 4 + k + 1) * capacity, columns
                            ] = got[
                                j * capacity : (j + 1) * capacity,
                                side * width : (side + 1) * width,
                            ]

    hidden = lax.dot_general(rows_ref[step], up_ref[0], NT, preferred_element_type=jnp.float32)
    activation = jnp.square(jnp.maximum(hidden, 0.0)).astype(jnp.bfloat16)
    out = jnp.dot(activation, down_ref[0], preferred_element_type=jnp.float32).astype(jnp.bfloat16)
    for r in range(4 * planes):
        terms_ref[r, at(step, capacity), :] = out[r * capacity : (r + 1) * capacity]

    @pl.when(step == count - 1)
    def _():
        for dc in range(2):
            for dy in range(planes):
                for dx in range(2):
                    block = spot ^ (dx * 2 + dc)
                    source = (plane ^ dy) * 4 + block
                    r = dy * 4 + (block ^ line)
                    out_refs[dc * sides + dy * 2 + dx][...] = jnp.dot(
                        gates_ref[source], terms_ref[r], preferred_element_type=jnp.float32
                    ).astype(jnp.bfloat16)


def experts(where, pieces, select, gates, up, down, capacity):
    count, units, latent = up.shape
    owners, tokens, _ = gates.shape
    sides = owners // 2
    shape = jax.ShapeDtypeStruct((tokens, latent), jnp.bfloat16)
    return pl.pallas_call(
        functools.partial(expert_kernel, sides, capacity),
        grid=(count,),
        in_specs=[SMEM]
        + [VMEM] * (len(pieces) + 2)
        + [
            pl.BlockSpec((1, units, latent), lambda i: (i, 0, 0)),
            pl.BlockSpec((1, units, latent), lambda i: (i, 0, 0)),
        ],
        out_specs=[VMEM] * owners,
        out_shape=[shape] * owners,
        scratch_shapes=[
            pltpu.VMEM((count, owners * capacity, latent), jnp.bfloat16),
            pltpu.VMEM((owners, count * capacity, latent), jnp.bfloat16),
        ],
        compiler_params=params(32),
        cost_estimate=pl.CostEstimate(
            flops=4 * count * owners * capacity * units * latent,
            bytes_accessed=4 * count * units * latent,
            transcendentals=0,
        ),
        name="experts",
    )(where, *pieces, select, gates, up, down)


def deal_kernel(where_ref, *refs):
    in_refs, out_refs = refs[:-4], refs[-4:]
    line = where_ref[2]
    share = out_refs[0].shape[0]
    for k in range(4):
        rows = at(line ^ k, share)
        total = in_refs[0][rows, :].astype(jnp.float32)
        for ref in in_refs[1:]:
            total = total + ref[rows, :].astype(jnp.float32)
        out_refs[k][...] = total.astype(jnp.bfloat16)


def deal(where, terms):
    tokens, latent = terms[0].shape
    shape = jax.ShapeDtypeStruct((tokens // 4, latent), jnp.bfloat16)
    return pl.pallas_call(
        deal_kernel,
        in_specs=[SMEM] + [VMEM] * len(terms),
        out_specs=[VMEM] * 4,
        out_shape=[shape] * 4,
        compiler_params=params(16),
        cost_estimate=pl.CostEstimate(flops=1 << 20, bytes_accessed=2 * MIB, transcendentals=0),
        name="deal",
    )(where, *terms)


def mixing_kernel(where_ref, *refs):
    parts, weight_refs, out_ref, rows_ref = refs[:4], refs[4:-2], refs[-2], refs[-1]
    line, owner = where_ref[2], where_ref[3]
    share = parts[0].shape[0]
    depth = rows_ref.shape[1] // len(weight_refs)
    for k in range(4):
        rows_ref[at(line ^ k, share), :] = parts[k][...]
    total = None
    for rel, weight_ref in enumerate(weight_refs):
        term = jnp.dot(
            rows_ref[:, at(owner ^ rel, depth)],
            weight_ref[0:depth, :],
            preferred_element_type=jnp.float32,
        )
        total = term if total is None else total + term
    out_ref[...] = total.astype(out_ref.dtype)


def mixing(where, parts, weights):
    share, latent = parts[0].shape
    columns = weights[0].shape[1]
    return pl.pallas_call(
        mixing_kernel,
        in_specs=[SMEM] + [VMEM] * (4 + len(weights)),
        out_specs=VMEM,
        out_shape=jax.ShapeDtypeStruct((share * 4, columns), jnp.bfloat16),
        scratch_shapes=[pltpu.VMEM((share * 4, latent), jnp.bfloat16)],
        compiler_params=params(16),
        cost_estimate=pl.CostEstimate(flops=1 << 28, bytes_accessed=3 * MIB, transcendentals=0),
        name="mixing",
    )(where, *parts, *weights)


def owner_move(value, offset, owners):
    return lax.ppermute(value, "expert", [(i, i ^ offset) for i in range(owners)])


def line_move(value, offset, line):
    return lax.ppermute(value, "hidden", [(i, i ^ offset) for i in range(line)])


def add(first, *others):
    total = first.astype(jnp.float32)
    for other in others:
        total = total + other.astype(jnp.float32)
    return total.astype(jnp.bfloat16)


def gathered(
    tokens, w_down, w1_values, w1_scales, w2_values, w2_scales, w_up, expert_ids, weight_codes
):
    owners, line = lax.axis_size("expert"), lax.axis_size("hidden")
    tok_rows, chosen = expert_ids.shape
    count = w1_values.shape[0]
    capacity = slots_of(tok_rows, chosen, count * owners)
    sides = owners // 2
    planes = owners // 4
    me, spot_z = lax.axis_index("expert"), lax.axis_index("hidden")
    where = jnp.stack([me // 4, me % 4, spot_z, me]).astype(jnp.int32)
    move = functools.partial(owner_move, owners=owners)
    slide = functools.partial(line_move, line=line)

    tok_side = move(tokens, 2)
    w_planes = [w_down] + [move(w_down, 4 * dy) for dy in range(1, planes)]
    tok_pair = move(tokens, 1)
    tok_cross = move(tok_side, 1)

    up = scale_weights(w1_values.swapaxes(1, 2), w1_scales.swapaxes(1, 2))
    down = scale_weights(w2_values, w2_scales)

    outs = latents(where, [tokens, tok_pair, tok_side, tok_cross], w_planes)
    share = add(outs[0], *[slide(outs[k], k) for k in range(1, line)])

    table = jnp.concatenate([expert_ids.T, weight_codes.T], axis=0).astype(jnp.bfloat16)
    table = jnp.pad(table, ((0, 16 - 2 * chosen), (0, w_up.shape[1] - tok_rows)))
    up_meta = jnp.concatenate([w_up, table], axis=0)
    up_meta, *_ = lax.optimization_barrier((up_meta, tok_side, *w_planes))
    metas = {0: up_meta}
    for d in range(1, sides):
        metas[2 * d] = move(up_meta, 2 * d)
    for d in range(sides):
        metas[2 * d + 1] = move(metas[2 * d], 1)
    metas = [metas[d] for d in range(owners)]
    select, gates = routing(where, metas, tok_rows, chosen, capacity, count)

    stack = jnp.stack([slide(share, k) for k in range(1, line)])
    pieces = {}
    for d in range(sides):
        pieces[2 * d] = (
            share if d == 0 else move(share, 2 * d),
            stack if d == 0 else move(stack, 2 * d),
        )
        pieces[2 * d + 1] = tuple(move(p, 1) for p in pieces[2 * d])
    flat = [p for d in range(owners) for p in pieces[d]]

    terms = experts(where, flat, select, gates, up, down, capacity)
    keep, send = terms[:sides], terms[sides:]
    held = [add(keep[d], move(send[d], 1)) for d in range(sides)]
    parts = deal(where, [held[0]] + [move(held[d], 2 * d) for d in range(1, sides)])
    own = add(parts[0], *[slide(parts[k], k) for k in range(1, line)])
    whole = [own] + [slide(own, k) for k in range(1, line)]
    return mixing(where, whole, metas)


def slots_of(tok_rows, chosen, total_experts):
    return max(2, (4 * tok_rows * chosen + 3 * total_experts - 1) // (3 * total_experts))


def exchanged(
    tokens, w_down, w1_values, w1_scales, w2_values, w2_scales, w_up, expert_ids, weight_codes
):
    tok_rows, chosen = expert_ids.shape
    local_count = w1_values.shape[0]
    owners = lax.axis_size("expert")
    total_experts = local_count * owners
    capacity = max(2, (4 * tok_rows * chosen + 3 * total_experts - 1) // (3 * total_experts))
    latent_width = w1_values.shape[1]
    flat_ids = expert_ids.reshape(-1)
    order = jnp.arange(tok_rows * chosen, dtype=jnp.int32)
    earlier = (flat_ids[:, None] == flat_ids[None, :]) & (order[:, None] > order[None, :])
    position = jnp.sum(earlier.astype(jnp.int32), axis=1)
    slot_index = (
        flat_ids % local_count * (owners * capacity) + flat_ids // local_count * capacity + position
    )
    source_row = order // chosen
    slot_table = (
        jnp.full((total_experts * capacity,), tok_rows, dtype=jnp.int32)
        .at[slot_index]
        .set(source_row)
    )
    partial_value = jnp.dot(
        tokens,
        lax.all_gather(w_down, "expert", axis=1, tiled=True),
        preferred_element_type=jnp.float32,
    )
    shares = lax.psum_scatter(
        partial_value.astype(jnp.bfloat16), "hidden", scatter_dimension=1, tiled=True
    )
    share_width = shares.shape[1]
    padded = jnp.concatenate([shares, jnp.zeros((1, share_width), dtype=jnp.bfloat16)], axis=0)
    outgoing = padded[slot_table].reshape(local_count, owners * capacity, share_width)
    moved_rows = lax.all_to_all(outgoing, "expert", split_axis=1, concat_axis=1, tiled=True)
    arrived = lax.all_gather(moved_rows, "hidden", axis=2, tiled=True)
    unit_count = w1_values.shape[2]
    blocks = w1_scales.shape[1]
    block_rows = latent_width // blocks
    up_weight = (
        (
            w1_values.reshape(local_count, blocks, block_rows, unit_count).astype(jnp.float32)
            * w1_scales[:, :, None, :]
        )
        .reshape(local_count, latent_width, unit_count)
        .astype(jnp.bfloat16)
    )
    down_weight = (
        (
            w2_values.reshape(local_count, unit_count, blocks, block_rows).astype(jnp.float32)
            * w2_scales[:, :, :, None]
        )
        .reshape(local_count, unit_count, latent_width)
        .astype(jnp.bfloat16)
    )
    hidden_pre = jnp.einsum("xsl,xlf->xsf", arrived, up_weight, preferred_element_type=jnp.float32)
    activation = jnp.square(jnp.maximum(hidden_pre, 0.0)).astype(jnp.bfloat16)
    expert_terms = jnp.einsum(
        "xsf,xfl->xsl", activation, down_weight, preferred_element_type=jnp.float32
    )
    code_values = weight_codes.astype(jnp.float32)
    gate = code_values / jnp.sum(code_values, axis=1, keepdims=True)
    expert_out = lax.psum_scatter(
        expert_terms.astype(jnp.bfloat16), "hidden", scatter_dimension=2, tiled=True
    ).astype(jnp.float32)
    returned = lax.all_to_all(
        expert_out.astype(jnp.bfloat16), "expert", split_axis=1, concat_axis=1, tiled=True
    ).astype(expert_out.dtype)
    share_width = returned.shape[2]
    flat_back = returned.reshape(total_experts * capacity, share_width)
    picked = flat_back[slot_index].reshape(tok_rows, chosen, share_width)
    combined = jnp.sum(picked * gate[:, :, None], axis=1).astype(jnp.bfloat16)
    whole = lax.all_gather(combined, "hidden", axis=1, tiled=True)
    result = jnp.dot(
        whole,
        lax.all_gather(w_up, "expert", axis=0, tiled=True),
        preferred_element_type=jnp.float32,
    )
    return result.astype(jnp.bfloat16)


def per_device(*args):
    tok_rows, chosen = args[7].shape
    owners, line = lax.axis_size("expert"), lax.axis_size("hidden")
    slots = args[2].shape[0] * owners * slots_of(tok_rows, chosen, args[2].shape[0] * owners)
    if owners * tok_rows <= slots and owners % 4 == 0 and owners & (owners - 1) == 0 and line == 4:
        return gathered(*args)
    return exchanged(*args)


def solution(mesh):
    placed = (
        P("expert", "hidden"),
        P("hidden", "expert"),
        P("expert", None, "hidden"),
        P("expert", None, "hidden"),
        P("expert", "hidden", None),
        P("expert", "hidden", None),
        P("expert", "hidden"),
        P("expert", None),
        P("expert", None),
    )
    return jax.shard_map(
        per_device, mesh=mesh, in_specs=placed, out_specs=P("expert", "hidden"), check_vma=False
    )
```
